32 devices in a mesh: row: 4 (over z), col: 8 (over y, x, core).
Axes of the slice: x: 2, y: 2, z: 4, core: 2. Of those that a mesh axis runs over, the one named last changes fastest.
Arguments:
- impedance: bfloat16 [2048, 2048], P('row', 'col'), may hold values from -2 to 50
- start: float32 [2048, 32], P(('row', 'col')), may hold values from -6 to 6
Outputs:
- basis: float32 [2048, 288], P(('row', 'col'))
- alphas: float32 [8, 32, 32], replicated
- betas: float32 [8, 32, 32], replicated
The draws below stay inside these ranges and needn't reach their ends.
All inputs are finite; a program needn't handle non-finite values.
Results may differ from the reference program's by a relative error of at most 0.039.
Values may be sent and summed in bfloat16 or wider, within the bound.
A program may use at most 64 MiB of HBM per device.

```python
import math
import jax
import jax.numpy as jnp
from jax import lax

P_SIZE = 32
STEPS = 8
N = 2048
N_ROW = 4


def draw_impedance(key, part):
    keys = jax.random.split(jax.random.fold_in(key, 11), 2)
    noise = jax.random.normal(keys[0], (N, N), jnp.float32)
    symmetric = (noise + noise.T) * (0.7 / math.sqrt(N))
    diagonal = jnp.exp(jax.random.uniform(keys[1], (N,), jnp.float32, math.log(2.5), math.log(12.0)))
    indices = jnp.arange(N)
    matrix = symmetric.at[indices, indices].add(diagonal)
    return matrix.astype(jnp.bfloat16)


def levels(rng, dims, cuts, smallest, largest):
    def one(dim, blocks):
        heights = jax.random.uniform(jax.random.fold_in(jax.random.fold_in(rng, 6), dim), (blocks,), jnp.float32, smallest / len(cuts), largest / len(cuts))
        return jnp.repeat(jnp.exp(heights), dims[dim] // blocks).reshape((-1,) + (1,) * (len(dims) - dim - 1))

    gain = one(*cuts[0])
    for cut in cuts[1:]:
        gain = gain * one(*cut)
    return gain


def gaussian(own_key, shape, deviation, bound, cuts=(), kind=jnp.bfloat16):
    array = deviation * jax.random.normal(own_key, shape, jnp.float32)
    if cuts:
        array = array * levels(own_key, shape, cuts, -0.22, 0.18)
    return jnp.clip(array, -bound, bound).astype(kind)


def setup_inputs(seed: int = 0) -> dict:
    arg_keys = jax.random.split(jax.random.key(seed), 3)
    return {
        "impedance": draw_impedance(jax.random.fold_in(arg_keys[2], 71), 0),
        "start": gaussian(arg_keys[1], (N, P_SIZE), 1.0, 6.0, ((0, 32),), jnp.float32),
    }


def orthonormal(block):
    gram = jnp.dot(block.T, block, precision=lax.Precision.HIGHEST)
    lower = jnp.linalg.cholesky(gram)
    return (jax.scipy.linalg.solve_triangular(lower, block.T, lower=True).T, lower)

def apply_matrix(impedance, vectors):
    column = vectors.astype(jnp.bfloat16).astype(jnp.float32)
    slabs = impedance.reshape(N_ROW, N // N_ROW, N)

    def one_slab(slab):
        return jnp.dot(slab.astype(jnp.float32), column, precision=lax.Precision.HIGHEST)
    return lax.map(one_slab, slabs).reshape(N, vectors.shape[1])

def reference(impedance, start):
    current, unused = orthonormal(start)
    basis_list = [current]
    alpha_list = []
    beta_list = []
    for step in range(STEPS):
        image = apply_matrix(impedance, current)
        stacked = jnp.concatenate(basis_list, axis=1)
        coeffs = jnp.dot(stacked.T, image, precision=lax.Precision.HIGHEST)
        residual = image - jnp.dot(stacked, coeffs, precision=lax.Precision.HIGHEST)
        current, lower = orthonormal(residual)
        alpha_list.append(coeffs[step * P_SIZE:(step + 1) * P_SIZE])
        beta_list.append(lower.T)
        basis_list.append(current)
    return (jnp.concatenate(basis_list, axis=1), jnp.stack(alpha_list), jnp.stack(beta_list))
```

```python
import functools

import jax
import jax.numpy as jnp
from jax import lax
from jax.experimental import pallas as pl
from jax.experimental.pallas import tpu as pltpu
from jax.sharding import PartitionSpec as P

STEPS = 8
LANES = 128
CHUNK = 2048
PANEL = 16
PARTS = 2
MESH = pl.DeviceIdType.MESH
f32 = jnp.float32
bf16 = jnp.bfloat16


def split(value):
    high = value.astype(bf16)
    return high, (value - high.astype(f32)).astype(bf16)


def across(left, right):
    return lax.dot_general(left, right, (((1,), (1,)), ((), ())), preferred_element_type=f32)


def over(trips, body, init):
    if trips == 1:
        return body(0, init)
    return lax.fori_loop(0, trips, body, init)


def factor(gram):
    width = gram.shape[0]
    rows = lax.broadcasted_iota(jnp.int32, (width, 2 * width), 0)
    lanes = lax.broadcasted_iota(jnp.int32, (width, 2 * width), 1)
    eye = (lanes - width == rows).astype(f32)
    work = jnp.where(lanes < width, jnp.concatenate([gram, gram], axis=1), eye)
    for base in range(0, width, PANEL):
        cols = [
            jnp.broadcast_to(work[:, base + m : base + m + 1], work.shape) for m in range(PANEL)
        ]
        for m in range(PANEL):
            k = base + m
            scale = 1.0 / cols[m][k : k + 1]
            mult = jnp.where(rows > k, cols[m] * scale, 0.0)
            work = work - mult * work[k : k + 1]
            for n in range(m + 1, PANEL):
                cols[n] = cols[n] - mult * cols[n][k : k + 1]
    diagonal = jnp.sum(jnp.where(lanes == rows, work, 0.0), axis=1, keepdims=True)
    work = work * lax.rsqrt(diagonal)
    upper = jnp.where(lanes >= rows, work, 0.0)[:, :width]
    return upper, work[:, width:]


def kernel(
    n_row, n_col, pair,
    imp_hbm, st_ref, basis_ref, alpha_ref, beta_ref,
    imp_ref,
    slab, tower, relay, parts, begin, image, high, low, res,
    a_send, a_recv, b_send, b_recv, d_send, d_recv, f_send, f_recv, imp_sem, p_send, p_recv, s_send, s_recv, i_send, i_recv,
):
    r = lax.axis_index("row")
    c = lax.axis_index("col")
    per_row = n_col // pair
    groups = n_row * per_row
    devices = n_row * n_col
    me = r * n_col + c
    group = r * per_row + c // pair
    member = c % pair
    width = st_ref.shape[0]
    cb = imp_ref.shape[1]
    total = image.shape[2]
    chunk = min(CHUNK, total)
    trips = total // chunk

    load = pltpu.make_async_copy(imp_hbm, imp_ref, imp_sem)
    load.start()
    barrier = pltpu.get_barrier_semaphore()
    for d in range(1, devices):
        t = (me + d) % devices
        pl.semaphore_signal(barrier, inc=1, device_id=(t // n_col, t % n_col), device_id_type=MESH)
    load.wait()
    pl.semaphore_wait(barrier, devices - 1)

    def lane_block(g):
        return pl.ds(pl.multiple_of(g * LANES, LANES), LANES)

    def row_block(k):
        size = per_row * LANES
        return pl.ds(pl.multiple_of(k * size, size), size)

    planes = n_row // 2
    side, level = r // planes, r % planes
    rows = imp_ref.shape[0]
    strips = cb // LANES

    def shift(value, offset, count, sign=1):
        if count & (count - 1):
            return (value + sign * offset + count) % count
        moved, bit = 0, 1
        while bit < count:
            moved = moved + (value // bit + offset // bit) % 2 * bit
            bit *= 2
        return moved

    def owned(z, x):
        return (z + x % 2 * planes) % n_row * per_row + x // 2

    def p_copy(q, owner):
        return pltpu.make_async_remote_copy(
            src_ref=st_ref, dst_ref=parts.at[owner],
            send_sem=p_send.at[q], recv_sem=p_recv.at[q],
            device_id=(r, c - member + (member + q) % pair), device_id_type=MESH,
        )

    near = sorted(range(n_row), key=lambda dz: min(dz, n_row - dz))
    slots = {dz: [dz * per_row + dx for dx in range(per_row) if dz or dx] for dz in near}
    near_first = [q for dz in near for q in reversed(slots[dz])]

    def peer(q):
        dz, dx = q // per_row, q % per_row
        return ((r + dz) % n_row, ((c // pair + dx) % per_row) * pair + member)

    def source(q):
        dz, dx = q // per_row, q % per_row
        return ((r + n_row - dz) % n_row) * per_row + (c // pair + per_row - dx) % per_row

    def st_copy(q, owner):
        where = begin.at[:, lane_block(owner)]
        return pltpu.make_async_remote_copy(
            src_ref=where, dst_ref=where, send_sem=s_send.at[q], recv_sem=s_recv.at[q],
            device_id=peer(q), device_id_type=MESH,
        )

    def a_copy(g):
        return pltpu.make_async_remote_copy(
            src_ref=imp_ref.at[g * LANES : (g + 1) * LANES, :], dst_ref=slab.at[c],
            send_sem=a_send.at[g], recv_sem=a_recv.at[c],
            device_id=(r, 2 * g), device_id_type=MESH,
        )

    k = c % 2
    lanes_of = [slice(s * LANES, (s + 1) * LANES) for s in range(strips)]
    hops = max(planes // 2, 1)

    def strip_target(s):
        g = c * strips + s
        return (g // per_row + planes) % n_row, g % per_row * 2 + 1

    def strip_relay(s):
        z, x = strip_target(s)
        return x - 1 + z % planes % 2

    def strip_local(s):
        z, x = strip_target(s)
        return (z == r) & (x == c)

    def strip_direct(s):
        z, x = strip_target(s)
        return ((z // planes == side) | (strip_relay(s) == c)) & jnp.logical_not(strip_local(s))

    def strip_relayed(s):
        return (strip_target(s)[0] // planes != side) & (strip_relay(s) != c)

    def b_copy(s):
        return pltpu.make_async_remote_copy(
            src_ref=imp_ref.at[:, lanes_of[s]], dst_ref=tower.at[r],
            send_sem=b_send.at[s], recv_sem=b_recv.at[r],
            device_id=strip_target(s), device_id_type=MESH,
        )

    def part(i):
        return slice(i * rows // PARTS, (i + 1) * rows // PARTS)

    def d_copy(s, i):
        slot = strip_target(s)[0] % planes // 2
        return pltpu.make_async_remote_copy(
            src_ref=imp_ref.at[part(i), lanes_of[s]], dst_ref=relay.at[slot, part(i)],
            send_sem=d_send.at[s, i], recv_sem=d_recv.at[slot, i],
            device_id=(r, strip_relay(s)), device_id_type=MESH,
        )

    def relay_target(slot):
        return (1 - side) * planes + slot * 2 + k, c // 2 * 2 + 1

    def relay_used(slot):
        z, x = relay_target(slot)
        g = (z + planes) % n_row * per_row + x // 2
        return (slot * 2 + k < planes) & (g // strips != c)

    def f_copy(slot, i):
        return pltpu.make_async_remote_copy(
            src_ref=relay.at[slot, part(i)], dst_ref=tower.at[r, part(i)],
            send_sem=f_send.at[slot, i], recv_sem=f_recv.at[r, i],
            device_id=relay_target(slot), device_id_type=MESH,
        )

    def d_wait(slot, i):
        where = relay.at[slot, part(i)]
        pltpu.make_async_remote_copy(
            src_ref=where, dst_ref=where, send_sem=f_send.at[slot, i], recv_sem=d_recv.at[slot, i],
            device_id=(r, c), device_id_type=MESH,
        ).wait_recv()

    def send_strip(s):
        for i in range(PARTS):
            d_copy(s, i).start()

    def sent_strip(s):
        for i in range(PARTS):
            d_copy(s, i).wait_send()

    def passed_on(slot):
        for i in range(PARTS):
            f_copy(slot, i).wait_send()

    def pass_on(slot, i):
        d_wait(slot, i)
        f_copy(slot, i).start()

    mine_at = owned(r, c)
    even = c % 2 == 0

    for s in range(strips):
        pl.when(strip_relayed(s))(functools.partial(send_strip, s))
    for q in range(1, pair):
        p_copy(q, member).start()
    for s in range(strips):
        pl.when(strip_direct(s))(b_copy(s).start)
    parts[member] = st_ref[...]
    for q in range(1, pair):
        p_copy(q, (member - q + pair) % pair).wait_recv()
    whole = parts[0]
    for p in range(1, pair):
        whole = whole + parts[p]
    begin[:, lane_block(group)] = whole
    for q in near_first:
        st_copy(q, group).start()
    for g in range(per_row):
        pl.when(c != 2 * g)(a_copy(g).start)
    for g in range(per_row):
        @pl.when(c == 2 * g)
        def _():
            slab[c] = imp_ref[g * LANES : (g + 1) * LANES, :]

    for s in range(strips):
        @pl.when(strip_local(s))
        def _():
            tower[r] = imp_ref[:, lanes_of[s]]

    for i in range(PARTS):
        for slot in range(hops):
            pl.when(relay_used(slot))(functools.partial(pass_on, slot, i))
    for q in range(1, groups):
        st_copy(q, source(q)).wait_recv()

    def orthonormal(block, index):
        def gram_chunk(i, gram):
            at = pl.ds(pl.multiple_of(i * chunk, chunk), chunk)
            h, l = split(block(at))
            res[0, :, at] = h
            res[1, :, at] = l
            both = across(jnp.concatenate([h, l], axis=0), h)
            return gram + (both[:width] + (both[width:] + both[width:].T))

        gram = over(trips, gram_chunk, jnp.zeros((width, width), f32))
        upper, inverse = factor(gram)
        ih, il = split(inverse)
        wide = jnp.concatenate([ih, ih, il], axis=1)

        def solve_chunk(i, carry):
            at = pl.ds(pl.multiple_of(i * chunk, chunk), chunk)
            h = res[0, :, at]
            tall = jnp.concatenate([h, res[1, :, at], h], axis=0)
            h, l = split(jnp.dot(wide, tall, preferred_element_type=f32))
            high[index * width : (index + 1) * width, at] = h
            low[index * width : (index + 1) * width, at] = l
            return carry

        over(trips, solve_chunk, 0)
        return upper

    def first(at):
        return begin[:, at].astype(f32)

    orthonormal(first, 0)

    def a_wait(x):
        pltpu.make_async_remote_copy(
            src_ref=slab.at[x], dst_ref=slab.at[x], send_sem=a_send.at[0], recv_sem=a_recv.at[x],
            device_id=(r, x), device_id_type=MESH,
        ).wait_recv()

    def b_wait(z):
        pltpu.make_async_remote_copy(
            src_ref=tower.at[z], dst_ref=tower.at[z], send_sem=b_send.at[0], recv_sem=b_recv.at[z],
            device_id=(z, c), device_id_type=MESH,
        ).wait_recv()

    for x in range(n_col):
        pl.when(even & (c != x))(functools.partial(a_wait, x))

    def t_wait(z, i):
        where = tower.at[z, part(i)]
        pltpu.make_async_remote_copy(
            src_ref=where, dst_ref=where, send_sem=f_send.at[0, i], recv_sem=f_recv.at[z, i],
            device_id=(z, c), device_id_type=MESH,
        ).wait_recv()

    def t_waits(z):
        for i in range(PARTS):
            t_wait(z, i)

    helper = c - 1 + level % 2
    for z in range(n_row):
        source = mine_at // strips
        far = (z // planes != side) & (source != helper)
        here = (source == c) & (z == r)
        pl.when((k == 1) & far)(functools.partial(t_waits, z))
        pl.when((k == 1) & jnp.logical_not(far) & jnp.logical_not(here))(functools.partial(b_wait, z))
    for q in range(1, pair):
        p_copy(q, member).wait_send()
    for q in range(1, groups):
        st_copy(q, group).wait_send()
    for g in range(per_row):
        pl.when(c != 2 * g)(a_copy(g).wait_send)
    for s in range(strips):
        pl.when(strip_direct(s))(b_copy(s).wait_send)
        pl.when(strip_relayed(s))(functools.partial(sent_strip, s))
    for slot in range(hops):
        pl.when(relay_used(slot))(functools.partial(passed_on, slot))

    offsets = [(dz, dc) for dz in reversed(range(planes)) for dc in reversed(range(n_col)) if dz or dc]

    def i_copy(par, dz, dc, owner):
        where = image.at[par, :, lane_block(owner)]
        index = dz * n_col + dc
        return pltpu.make_async_remote_copy(
            src_ref=where, dst_ref=where,
            send_sem=i_send.at[par, index], recv_sem=i_recv.at[par, index],
            device_id=(side * planes + shift(level, dz, planes), shift(c, dc, n_col)),
            device_id_type=MESH,
        )

    def i_wait(par, dz, dc):
        z = side * planes + shift(level, dz, planes, -1)
        i_copy(par, dz, dc, owned(z, shift(c, dc, n_col, -1))).wait_recv()

    for step in range(STEPS):
        par = step % 2
        seen = (step + 1) * width
        now = slice(step * width, seen)

        @pl.when(even)
        def _():
            mine = jnp.zeros((width, LANES), f32)
            for x in range(n_col):
                mine = mine + across(high[now, x * cb : (x + 1) * cb], slab[x])
            image[par, :, lane_block(mine_at)] = mine.astype(image.dtype)

        @pl.when(c % 2 == 1)
        def _():
            mine = jnp.zeros((width, LANES), f32)
            for z in range(n_row):
                mine = mine + jnp.dot(
                    high[now, z * rows : (z + 1) * rows], tower[z], preferred_element_type=f32
                )
            image[par, :, lane_block(mine_at)] = mine.astype(image.dtype)

        for dz, dc in offsets:
            i_copy(par, dz, dc, mine_at).start()
        coeffs = jnp.zeros((width, seen), f32)
        for dz in range(planes):
            for there in [dc for z, dc in reversed(offsets) if z == dz]:
                i_wait(par, dz, there)
            base = shift(level, dz, planes, -1)
            for half in range(2):
                at = row_block(base + half * planes)
                h = image[par, :, at]
                coeffs = coeffs + across(h, high[:seen, at]) + across(h, low[:seen, at])
        ch, cl = split(coeffs)
        c_both = jnp.concatenate([ch, cl], axis=0)

        def residual(at):
            both = jnp.dot(c_both, high[:seen, at], preferred_element_type=f32)
            fix = jnp.dot(ch, low[:seen, at], preferred_element_type=f32)
            return image[par, :, at].astype(f32) - (both[:width] + both[width:] + fix)

        beta_ref[step] = orthonormal(residual, step + 1)
        alpha_ref[step] = coeffs[:, step * width : seen].T
        for dz, dc in offsets:
            i_copy(par, dz, dc, mine_at).wait_send()

    own = lane_block(group)
    basis_ref[...] = high[:, own].astype(f32) + low[:, own].astype(f32)


def local(impedance, start):
    n_row, n_col = lax.axis_size("row"), lax.axis_size("col")
    share, width = start.shape
    pair = LANES // share
    total = share * n_row * n_col
    groups = total // LANES
    blocks = (STEPS + 1) * width
    member = lax.axis_index("col") % pair
    lanes = lax.broadcasted_iota(jnp.int32, (width, LANES), 1)
    placed = jnp.where(lanes // share == member, jnp.concatenate([start.T] * pair, axis=1), 0.0)
    placed = placed.astype(bf16)
    hops = max(n_row // 4, 1)
    vmem = pl.BlockSpec(memory_space=pltpu.VMEM)
    dma = pltpu.SemaphoreType.DMA
    basis, alphas, betas = pl.pallas_call(
        functools.partial(kernel, n_row, n_col, pair),
        out_shape=(
            jax.ShapeDtypeStruct((blocks, LANES), f32),
            jax.ShapeDtypeStruct((STEPS, width, width), f32),
            jax.ShapeDtypeStruct((STEPS, width, width), f32),
        ),
        in_specs=[pl.BlockSpec(memory_space=pl.ANY), vmem],
        out_specs=(vmem, vmem, vmem),
        scratch_shapes=[
            pltpu.VMEM(impedance.shape, bf16),
            pltpu.VMEM((n_col, LANES, impedance.shape[1]), bf16),
            pltpu.VMEM((n_row, impedance.shape[0], LANES), bf16),
            pltpu.VMEM((hops, impedance.shape[0], LANES), bf16),
            pltpu.VMEM((pair, width, LANES), bf16),
            pltpu.VMEM((width, total), bf16),
            pltpu.VMEM((2, width, total), bf16),
            pltpu.VMEM((blocks, total), bf16),
            pltpu.VMEM((blocks, total), bf16),
            pltpu.VMEM((2, width, total), bf16),
            dma((n_col // 2,)), dma((n_col,)),
            dma((impedance.shape[1] // LANES,)), dma((n_row,)),
            dma((impedance.shape[1] // LANES, PARTS)), dma((hops, PARTS)),
            dma((hops, PARTS)), dma((n_row, PARTS)), dma,
            dma((pair,)), dma((pair,)),
            dma((groups,)), dma((groups,)),
            dma((2, groups)), dma((2, groups)),
        ],
        compiler_params=pltpu.CompilerParams(
            collective_id=0, has_side_effects=True, vmem_limit_bytes=60 * 1024 * 1024
        ),
    )(impedance, placed)
    mine = lax.dynamic_slice_in_dim(basis, member * share, share, 1)
    return mine.T, alphas, betas


def solution(mesh):
    return jax.shard_map(
        local,
        mesh=mesh,
        in_specs=(P("row", "col"), P(("row", "col"), None)),
        out_specs=(P(("row", "col"), None), P(), P()),
        check_vma=False,
    )
```

```python
import functools

import jax
import jax.numpy as jnp
from jax import lax
from jax.experimental import pallas as pl
from jax.experimental.pallas import tpu as pltpu
from jax.sharding import PartitionSpec as P

STEPS = 8
LANES = 128
CHUNK = 2048
PANEL = 16
PARTS = 2
MESH = pl.DeviceIdType.MESH
f32 = jnp.float32
bf16 = jnp.bfloat16


def split(value):
    high = value.astype(bf16)
    return high, (value - high.astype(f32)).astype(bf16)


def across(left, right):
    return lax.dot_general(left, right, (((1,), (1,)), ((), ())), preferred_element_type=f32)


def over(trips, body, init):
    if trips == 1:
        return body(0, init)
    return lax.fori_loop(0, trips, body, init)


def factor(gram):
    width = gram.shape[0]
    rows = lax.broadcasted_iota(jnp.int32, (width, 2 * width), 0)
    lanes = lax.broadcasted_iota(jnp.int32, (width, 2 * width), 1)
    eye = (lanes - width == rows).astype(f32)
    work = jnp.where(lanes < width, jnp.concatenate([gram, gram], axis=1), eye)
    for base in range(0, width, PANEL):
        cols = [
            jnp.broadcast_to(work[:, base + m : base + m + 1], work.shape) for m in range(PANEL)
        ]
        for m in range(PANEL):
            k = base + m
            scale = 1.0 / cols[m][k : k + 1]
            mult = jnp.where(rows > k, cols[m] * scale, 0.0)
            work = work - mult * work[k : k + 1]
            for n in range(m + 1, PANEL):
                cols[n] = cols[n] - mult * cols[n][k : k + 1]
    diagonal = jnp.sum(jnp.where(lanes == rows, work, 0.0), axis=1, keepdims=True)
    work = work * lax.rsqrt(diagonal)
    upper = jnp.where(lanes >= rows, work, 0.0)[:, :width]
    return upper, work[:, width:]


def kernel(
    n_row, n_col, pair,
    imp_hbm, start_ref, basis_ref, alpha_ref, beta_ref,
    imp_ref, st_ref,
    slab, tower, relay, parts, begin, image, high, low, res,
    a_send, a_recv, b_send, b_recv, d_send, d_recv, f_send, f_recv, imp_sem, p_send, p_recv, s_send, s_recv, i_send, i_recv,
):
    r = lax.axis_index("row")
    c = lax.axis_index("col")
    per_row = n_col // pair
    groups = n_row * per_row
    devices = n_row * n_col
    me = r * n_col + c
    group = r * per_row + c // pair
    member = c % pair
    width, share = start_ref.shape
    cb = imp_ref.shape[1]
    total = image.shape[2]
    chunk = min(CHUNK, total)
    trips = total // chunk

    load = pltpu.make_async_copy(imp_hbm, imp_ref, imp_sem)
    load.start()
    barrier = pltpu.get_barrier_semaphore()
    for d in range(1, devices):
        t = (me + d) % devices
        pl.semaphore_signal(barrier, inc=1, device_id=(t // n_col, t % n_col), device_id_type=MESH)
    turned = start_ref[...]
    lanes = lax.broadcasted_iota(jnp.int32, (width, LANES), 1)
    placed = jnp.where(lanes // share == member, jnp.concatenate([turned] * pair, axis=1), 0.0)
    st_ref[...] = placed.astype(bf16)
    load.wait()
    pl.semaphore_wait(barrier, devices - 1)

    def lane_block(g):
        return pl.ds(pl.multiple_of(g * LANES, LANES), LANES)

    def row_block(k):
        size = per_row * LANES
        return pl.ds(pl.multiple_of(k * size, size), size)

    planes = n_row // 2
    side, level = r // planes, r % planes
    rows = imp_ref.shape[0]
    strips = cb // LANES

    def shift(value, offset, count, sign=1):
        if count & (count - 1):
            return (value + sign * offset + count) % count
        moved, bit = 0, 1
        while bit < count:
            moved = moved + (value // bit + offset // bit) % 2 * bit
            bit *= 2
        return moved

    share_of = per_row // planes

    def owned(z, x):
        q = x // 2
        far = (1 - z // planes) * planes + q % planes
        other = far * per_row + z % planes * share_of + q // planes
        return x % 2 * other + (1 - x % 2) * (z * per_row + q)

    def p_copy(q, owner):
        return pltpu.make_async_remote_copy(
            src_ref=st_ref, dst_ref=parts.at[owner],
            send_sem=p_send.at[q], recv_sem=p_recv.at[q],
            device_id=(r, c - member + (member + q) % pair), device_id_type=MESH,
        )

    near = sorted(range(n_row), key=lambda dz: min(dz, n_row - dz))
    slots = {dz: [dz * per_row + dx for dx in range(per_row) if dz or dx] for dz in near}
    near_first = [q for dz in near for q in reversed(slots[dz])]

    def peer(q):
        dz, dx = q // per_row, q % per_row
        return ((r + dz) % n_row, ((c // pair + dx) % per_row) * pair + member)

    def source(q):
        dz, dx = q // per_row, q % per_row
        return ((r + n_row - dz) % n_row) * per_row + (c // pair + per_row - dx) % per_row

    def st_copy(q, owner):
        where = begin.at[:, lane_block(owner)]
        return pltpu.make_async_remote_copy(
            src_ref=where, dst_ref=where, send_sem=s_send.at[q], recv_sem=s_recv.at[q],
            device_id=peer(q), device_id_type=MESH,
        )

    def a_copy(g):
        return pltpu.make_async_remote_copy(
            src_ref=imp_ref.at[g * LANES : (g + 1) * LANES, :], dst_ref=slab.at[c],
            send_sem=a_send.at[g], recv_sem=a_recv.at[c],
            device_id=(r, 2 * g), device_id_type=MESH,
        )

    k = c % 2
    lanes_of = [slice(s * LANES, (s + 1) * LANES) for s in range(strips)]
    hops = max(planes // 2, 1)

    def strip_target(s):
        g = c * strips + s
        z, at = g // per_row, g % per_row
        q = at % share_of * planes + z % planes
        return (1 - z // planes) * planes + at // share_of, q * 2 + 1

    def strip_relay(s):
        z, x = strip_target(s)
        return x - 1 + z % planes % 2

    def strip_local(s):
        z, x = strip_target(s)
        return (z == r) & (x == c)

    def strip_direct(s):
        z, x = strip_target(s)
        return ((z // planes == side) | (strip_relay(s) == c)) & jnp.logical_not(strip_local(s))

    def strip_relayed(s):
        return (strip_target(s)[0] // planes != side) & (strip_relay(s) != c)

    def b_copy(s):
        return pltpu.make_async_remote_copy(
            src_ref=imp_ref.at[:, lanes_of[s]], dst_ref=tower.at[r],
            send_sem=b_send.at[s], recv_sem=b_recv.at[r],
            device_id=strip_target(s), device_id_type=MESH,
        )

    def part(i):
        return slice(i * rows // PARTS, (i + 1) * rows // PARTS)

    def d_copy(s, i):
        slot = strip_target(s)[0] % planes // 2
        return pltpu.make_async_remote_copy(
            src_ref=imp_ref.at[part(i), lanes_of[s]], dst_ref=relay.at[slot, part(i)],
            send_sem=d_send.at[s, i], recv_sem=d_recv.at[slot, i],
            device_id=(r, strip_relay(s)), device_id_type=MESH,
        )

    def relay_target(slot):
        return (1 - side) * planes + slot * 2 + k, c // 2 * 2 + 1

    def relay_used(slot):
        return (slot * 2 + k < planes) & (owned(*relay_target(slot)) // strips != c)

    def f_copy(slot, i):
        return pltpu.make_async_remote_copy(
            src_ref=relay.at[slot, part(i)], dst_ref=tower.at[r, part(i)],
            send_sem=f_send.at[slot, i], recv_sem=f_recv.at[r, i],
            device_id=relay_target(slot), device_id_type=MESH,
        )

    def d_wait(slot, i):
        where = relay.at[slot, part(i)]
        pltpu.make_async_remote_copy(
            src_ref=where, dst_ref=where, send_sem=f_send.at[slot, i], recv_sem=d_recv.at[slot, i],
            device_id=(r, c), device_id_type=MESH,
        ).wait_recv()

    def send_strip(s):
        for i in range(PARTS):
            d_copy(s, i).start()

    def sent_strip(s):
        for i in range(PARTS):
            d_copy(s, i).wait_send()

    def passed_on(slot):
        for i in range(PARTS):
            f_copy(slot, i).wait_send()

    def pass_on(slot, i):
        d_wait(slot, i)
        f_copy(slot, i).start()

    mine_at = owned(r, c)
    even = c % 2 == 0

    for s in range(strips):
        pl.when(strip_relayed(s))(functools.partial(send_strip, s))
    for q in range(1, pair):
        p_copy(q, member).start()
    for s in range(strips):
        pl.when(strip_direct(s))(b_copy(s).start)
    parts[member] = st_ref[...]
    for q in range(1, pair):
        p_copy(q, (member - q + pair) % pair).wait_recv()
    whole = parts[0]
    for p in range(1, pair):
        whole = whole + parts[p]
    begin[:, lane_block(group)] = whole
    for q in near_first:
        st_copy(q, group).start()
    for g in range(per_row):
        pl.when(c != 2 * g)(a_copy(g).start)
    for g in range(per_row):
        @pl.when(c == 2 * g)
        def _():
            slab[c] = imp_ref[g * LANES : (g + 1) * LANES, :]

    for s in range(strips):
        @pl.when(strip_local(s))
        def _():
            tower[r] = imp_ref[:, lanes_of[s]]

    for i in range(PARTS):
        for slot in range(hops):
            pl.when(relay_used(slot))(functools.partial(pass_on, slot, i))
    for q in range(1, groups):
        st_copy(q, source(q)).wait_recv()

    def orthonormal(block, index):
        def gram_chunk(i, gram):
            at = pl.ds(pl.multiple_of(i * chunk, chunk), chunk)
            h, l = split(block(at))
            res[0, :, at] = h
            res[1, :, at] = l
            both = across(jnp.concatenate([h, l], axis=0), h)
            return gram + (both[:width] + (both[width:] + both[width:].T))

        gram = over(trips, gram_chunk, jnp.zeros((width, width), f32))
        upper, inverse = factor(gram)
        ih, il = split(inverse)
        wide = jnp.concatenate([ih, ih, il], axis=1)

        def solve_chunk(i, carry):
            at = pl.ds(pl.multiple_of(i * chunk, chunk), chunk)
            h = res[0, :, at]
            tall = jnp.concatenate([h, res[1, :, at], h], axis=0)
            h, l = split(jnp.dot(wide, tall, preferred_element_type=f32))
            high[index * width : (index + 1) * width, at] = h
            low[index * width : (index + 1) * width, at] = l
            return carry

        over(trips, solve_chunk, 0)
        return upper

    def first(at):
        return begin[:, at].astype(f32)

    orthonormal(first, 0)

    def a_wait(x):
        pltpu.make_async_remote_copy(
            src_ref=slab.at[x], dst_ref=slab.at[x], send_sem=a_send.at[0], recv_sem=a_recv.at[x],
            device_id=(r, x), device_id_type=MESH,
        ).wait_recv()

    def b_wait(z):
        pltpu.make_async_remote_copy(
            src_ref=tower.at[z], dst_ref=tower.at[z], send_sem=b_send.at[0], recv_sem=b_recv.at[z],
            device_id=(z, c), device_id_type=MESH,
        ).wait_recv()

    for x in range(n_col):
        pl.when(even & (c != x))(functools.partial(a_wait, x))

    def t_wait(z, i):
        where = tower.at[z, part(i)]
        pltpu.make_async_remote_copy(
            src_ref=where, dst_ref=where, send_sem=f_send.at[0, i], recv_sem=f_recv.at[z, i],
            device_id=(z, c), device_id_type=MESH,
        ).wait_recv()

    def t_waits(z):
        for i in range(PARTS):
            t_wait(z, i)

    helper = c - 1 + level % 2
    for z in range(n_row):
        source = mine_at // strips
        far = (z // planes != side) & (source != helper)
        here = (source == c) & (z == r)
        pl.when((k == 1) & far)(functools.partial(t_waits, z))
        pl.when((k == 1) & jnp.logical_not(far) & jnp.logical_not(here))(functools.partial(b_wait, z))
    for q in range(1, pair):
        p_copy(q, member).wait_send()
    for q in range(1, groups):
        st_copy(q, group).wait_send()
    for g in range(per_row):
        pl.when(c != 2 * g)(a_copy(g).wait_send)
    for s in range(strips):
        pl.when(strip_direct(s))(b_copy(s).wait_send)
        pl.when(strip_relayed(s))(functools.partial(sent_strip, s))
    for slot in range(hops):
        pl.when(relay_used(slot))(functools.partial(passed_on, slot))

    offsets = [(dz, dc) for dz in reversed(range(planes)) for dc in reversed(range(n_col)) if dz or dc]

    def i_copy(par, dz, dc, owner):
        where = image.at[par, :, lane_block(owner)]
        index = dz * n_col + dc
        return pltpu.make_async_remote_copy(
            src_ref=where, dst_ref=where,
            send_sem=i_send.at[par, index], recv_sem=i_recv.at[par, index],
            device_id=(side * planes + shift(level, dz, planes), shift(c, dc, n_col)),
            device_id_type=MESH,
        )

    def i_wait(par, dz, dc):
        z = side * planes + shift(level, dz, planes, -1)
        i_copy(par, dz, dc, owned(z, shift(c, dc, n_col, -1))).wait_recv()

    def turn(index):
        at = slice(index * width, (index + 1) * width)
        own = lane_block(group)
        value = high[at, own].astype(f32) + low[at, own].astype(f32)
        out = value[:, :share]
        for i in range(1, pair):
            out = jnp.where(member == i, value[:, i * share : (i + 1) * share], out)
        basis_ref[at, :] = out

    for step in range(STEPS):
        par = step % 2
        seen = (step + 1) * width
        now = slice(step * width, seen)

        @pl.when(even)
        def _():
            mine = jnp.zeros((width, LANES), f32)
            for x in range(n_col):
                mine = mine + across(high[now, x * cb : (x + 1) * cb], slab[x])
            image[par, :, lane_block(mine_at)] = mine.astype(image.dtype)

        @pl.when(c % 2 == 1)
        def _():
            mine = jnp.zeros((width, LANES), f32)
            for z in range(n_row):
                mine = mine + jnp.dot(
                    high[now, z * rows : (z + 1) * rows], tower[z], preferred_element_type=f32
                )
            image[par, :, lane_block(mine_at)] = mine.astype(image.dtype)

        for dz, dc in offsets:
            i_copy(par, dz, dc, mine_at).start()
        turn(step)
        coeffs = jnp.zeros((width, seen), f32)
        for dz in range(planes):
            for there in [dc for z, dc in reversed(offsets) if z == dz]:
                i_wait(par, dz, there)
            base = shift(level, dz, planes, -1)
            spots = [row_block(side * planes + base)]
            size = share_of * LANES
            for i in range(planes):
                far = ((1 - side) * planes + i) * per_row + base * share_of
                spots.append(pl.ds(pl.multiple_of(far * LANES, size), size))
            for at in spots:
                h = image[par, :, at]
                coeffs = coeffs + across(h, high[:seen, at]) + across(h, low[:seen, at])
        ch, cl = split(coeffs)
        c_both = jnp.concatenate([ch, cl], axis=0)

        def residual(at):
            both = jnp.dot(c_both, high[:seen, at], preferred_element_type=f32)
            fix = jnp.dot(ch, low[:seen, at], preferred_element_type=f32)
            return image[par, :, at].astype(f32) - (both[:width] + both[width:] + fix)

        beta_ref[step] = orthonormal(residual, step + 1)
        alpha_ref[step] = coeffs[:, step * width : seen].T
        for dz, dc in offsets:
            i_copy(par, dz, dc, mine_at).wait_send()

    turn(STEPS)


def local(impedance, start):
    n_row, n_col = lax.axis_size("row"), lax.axis_size("col")
    share, width = start.shape
    pair = LANES // share
    total = share * n_row * n_col
    groups = total // LANES
    blocks = (STEPS + 1) * width
    hops = max(n_row // 4, 1)
    vmem = pl.BlockSpec(memory_space=pltpu.VMEM)
    dma = pltpu.SemaphoreType.DMA
    basis, alphas, betas = pl.pallas_call(
        functools.partial(kernel, n_row, n_col, pair),
        out_shape=(
            jax.ShapeDtypeStruct((blocks, share), f32),
            jax.ShapeDtypeStruct((STEPS, width, width), f32),
            jax.ShapeDtypeStruct((STEPS, width, width), f32),
        ),
        in_specs=[pl.BlockSpec(memory_space=pl.ANY), vmem],
        out_specs=(vmem, vmem, vmem),
        scratch_shapes=[
            pltpu.VMEM(impedance.shape, bf16),
            pltpu.VMEM((width, LANES), bf16),
            pltpu.VMEM((n_col, LANES, impedance.shape[1]), bf16),
            pltpu.VMEM((n_row, impedance.shape[0], LANES), bf16),
            pltpu.VMEM((hops, impedance.shape[0], LANES), bf16),
            pltpu.VMEM((pair, width, LANES), bf16),
            pltpu.VMEM((width, total), bf16),
            pltpu.VMEM((2, width, total), bf16),
            pltpu.VMEM((blocks, total), bf16),
            pltpu.VMEM((blocks, total), bf16),
            pltpu.VMEM((2, width, total), bf16),
            dma((n_col // 2,)), dma((n_col,)),
            dma((impedance.shape[1] // LANES,)), dma((n_row,)),
            dma((impedance.shape[1] // LANES, PARTS)), dma((hops, PARTS)),
            dma((hops, PARTS)), dma((n_row, PARTS)), dma,
            dma((pair,)), dma((pair,)),
            dma((groups,)), dma((groups,)),
            dma((2, groups)), dma((2, groups)),
        ],
        compiler_params=pltpu.CompilerParams(
            collective_id=0, has_side_effects=True, vmem_limit_bytes=60 * 1024 * 1024
        ),
    )(impedance, start.T)
    return basis.T, alphas, betas


def solution(mesh):
    return jax.shard_map(
        local,
        mesh=mesh,
        in_specs=(P("row", "col"), P(("row", "col"), None)),
        out_specs=(P(("row", "col"), None), P(), P()),
        check_vma=False,
    )
```

```python
import functools

import jax
import jax.numpy as jnp
from jax import lax
from jax.experimental import pallas as pl
from jax.experimental.pallas import tpu as pltpu
from jax.sharding import PartitionSpec as P

STEPS = 8
LANES = 128
CHUNK = 2048
PANEL = 16
PARTS = 2
MESH = pl.DeviceIdType.MESH
f32 = jnp.float32
bf16 = jnp.bfloat16


def split(value):
    high = value.astype(bf16)
    return high, (value - high.astype(f32)).astype(bf16)


def across(left, right):
    return lax.dot_general(left, right, (((1,), (1,)), ((), ())), preferred_element_type=f32)


def over(trips, body, init):
    if trips == 1:
        return body(0, init)
    return lax.fori_loop(0, trips, body, init)


def factor(gram):
    width = gram.shape[0]
    rows = lax.broadcasted_iota(jnp.int32, (width, 2 * width), 0)
    lanes = lax.broadcasted_iota(jnp.int32, (width, 2 * width), 1)
    eye = (lanes - width == rows).astype(f32)
    work = jnp.where(lanes < width, jnp.concatenate([gram, gram], axis=1), eye)
    for base in range(0, width, PANEL):
        cols = [
            jnp.broadcast_to(work[:, base + m : base + m + 1], work.shape) for m in range(PANEL)
        ]
        for m in range(PANEL):
            k = base + m
            scale = 1.0 / cols[m][k : k + 1]
            mult = jnp.where(rows > k, cols[m] * scale, 0.0)
            work = work - mult * work[k : k + 1]
            for n in range(m + 1, PANEL):
                cols[n] = cols[n] - mult * cols[n][k : k + 1]
    diagonal = jnp.sum(jnp.where(lanes == rows, work, 0.0), axis=1, keepdims=True)
    work = work * lax.rsqrt(diagonal)
    upper = jnp.where(lanes >= rows, work, 0.0)[:, :width]
    return upper, work[:, width:]


def kernel(
    n_row, n_col, pair,
    imp_hbm, start_ref, basis_ref, alpha_ref, beta_ref,
    imp_ref, st_ref,
    slab, tower, relay, parts, begin, image, high, low, res,
    a_send, a_recv, b_send, b_recv, d_send, d_recv, f_send, f_recv, imp_sem, p_send, p_recv, s_send, s_recv, i_send, i_recv,
):
    r = lax.axis_index("row")
    c = lax.axis_index("col")
    per_row = n_col // pair
    groups = n_row * per_row
    devices = n_row * n_col
    me = r * n_col + c
    group = r * per_row + c // pair
    member = c % pair
    width, share = start_ref.shape
    cb = imp_ref.shape[1]
    total = image.shape[2]
    chunk = min(CHUNK, total)
    trips = total // chunk

    load = pltpu.make_async_copy(imp_hbm, imp_ref, imp_sem)
    load.start()
    barrier = pltpu.get_barrier_semaphore()
    for d in range(1, devices):
        t = (me + d) % devices
        pl.semaphore_signal(barrier, inc=1, device_id=(t // n_col, t % n_col), device_id_type=MESH)
    turned = start_ref[...]
    lanes = lax.broadcasted_iota(jnp.int32, (width, LANES), 1)
    placed = jnp.where(lanes // share == member, jnp.concatenate([turned] * pair, axis=1), 0.0)
    st_ref[...] = placed.astype(bf16)
    load.wait()
    pl.semaphore_wait(barrier, devices - 1)

    def lane_block(g):
        return pl.ds(pl.multiple_of(g * LANES, LANES), LANES)

    def row_block(k):
        size = per_row * LANES
        return pl.ds(pl.multiple_of(k * size, size), size)

    planes = n_row // 2
    side, level = r // planes, r % planes
    rows = imp_ref.shape[0]
    strips = cb // LANES

    def shift(value, offset, count, sign=1):
        if count & (count - 1):
            return (value + sign * offset + count) % count
        moved, bit = 0, 1
        while bit < count:
            moved = moved + (value // bit + offset // bit) % 2 * bit
            bit *= 2
        return moved

    share_of = per_row // planes

    def owned(z, x):
        q = x // 2
        far = (1 - z // planes) * planes + q % planes
        other = far * per_row + z % planes * share_of + q // planes
        return x % 2 * other + (1 - x % 2) * (z * per_row + q)

    def p_copy(q, owner):
        return pltpu.make_async_remote_copy(
            src_ref=st_ref, dst_ref=parts.at[owner],
            send_sem=p_send.at[q], recv_sem=p_recv.at[q],
            device_id=(r, c - member + (member + q) % pair), device_id_type=MESH,
        )

    near = sorted(range(n_row), key=lambda dz: min(dz, n_row - dz))
    slots = {dz: [dz * per_row + dx for dx in range(per_row) if dz or dx] for dz in near}
    near_first = [q for dz in near for q in reversed(slots[dz])]

    def peer(q):
        dz, dx = q // per_row, q % per_row
        return ((r + dz) % n_row, ((c // pair + dx) % per_row) * pair + member)

    def source(q):
        dz, dx = q // per_row, q % per_row
        return ((r + n_row - dz) % n_row) * per_row + (c // pair + per_row - dx) % per_row

    def st_copy(q, owner):
        where = begin.at[:, lane_block(owner)]
        return pltpu.make_async_remote_copy(
            src_ref=where, dst_ref=where, send_sem=s_send.at[q], recv_sem=s_recv.at[q],
            device_id=peer(q), device_id_type=MESH,
        )

    def a_copy(g):
        return pltpu.make_async_remote_copy(
            src_ref=imp_ref.at[g * LANES : (g + 1) * LANES, :], dst_ref=slab.at[c],
            send_sem=a_send.at[g], recv_sem=a_recv.at[c],
            device_id=(r, 2 * g), device_id_type=MESH,
        )

    k = c % 2
    lanes_of = [slice(s * LANES, (s + 1) * LANES) for s in range(strips)]
    hops = max(planes // 2, 1)

    def strip_target(s):
        g = c * strips + s
        z, at = g // per_row, g % per_row
        q = at % share_of * planes + z % planes
        return (1 - z // planes) * planes + at // share_of, q * 2 + 1

    def strip_relay(s):
        z, x = strip_target(s)
        return x - 1 + z % planes % 2

    def strip_local(s):
        z, x = strip_target(s)
        return (z == r) & (x == c)

    def strip_direct(s):
        z, x = strip_target(s)
        return ((z // planes == side) | (strip_relay(s) == c)) & jnp.logical_not(strip_local(s))

    def strip_relayed(s):
        return (strip_target(s)[0] // planes != side) & (strip_relay(s) != c)

    def b_copy(s):
        return pltpu.make_async_remote_copy(
            src_ref=imp_ref.at[:, lanes_of[s]], dst_ref=tower.at[r],
            send_sem=b_send.at[s], recv_sem=b_recv.at[r],
            device_id=strip_target(s), device_id_type=MESH,
        )

    def part(i):
        return slice(i * rows // PARTS, (i + 1) * rows // PARTS)

    def d_copy(s, i):
        slot = strip_target(s)[0] % planes // 2
        return pltpu.make_async_remote_copy(
            src_ref=imp_ref.at[part(i), lanes_of[s]], dst_ref=relay.at[slot, part(i)],
            send_sem=d_send.at[s, i], recv_sem=d_recv.at[slot, i],
            device_id=(r, strip_relay(s)), device_id_type=MESH,
        )

    def relay_target(slot):
        return (1 - side) * planes + slot * 2 + k, c // 2 * 2 + 1

    def relay_used(slot):
        return (slot * 2 + k < planes) & (owned(*relay_target(slot)) // strips != c)

    def f_copy(slot, i):
        return pltpu.make_async_remote_copy(
            src_ref=relay.at[slot, part(i)], dst_ref=tower.at[r, part(i)],
            send_sem=f_send.at[slot, i], recv_sem=f_recv.at[r, i],
            device_id=relay_target(slot), device_id_type=MESH,
        )

    def d_wait(slot, i):
        where = relay.at[slot, part(i)]
        pltpu.make_async_remote_copy(
            src_ref=where, dst_ref=where, send_sem=f_send.at[slot, i], recv_sem=d_recv.at[slot, i],
            device_id=(r, c), device_id_type=MESH,
        ).wait_recv()

    def send_strip(s):
        for i in range(PARTS):
            d_copy(s, i).start()

    def sent_strip(s):
        for i in range(PARTS):
            d_copy(s, i).wait_send()

    def passed_on(slot):
        for i in range(PARTS):
            f_copy(slot, i).wait_send()

    def pass_on(slot, i):
        d_wait(slot, i)
        f_copy(slot, i).start()

    mine_at = owned(r, c)
    even = c % 2 == 0

    for s in range(strips):
        pl.when(strip_relayed(s))(functools.partial(send_strip, s))
    for q in range(1, pair):
        p_copy(q, member).start()
    parts[member] = st_ref[...]
    for q in range(1, pair):
        p_copy(q, (member - q + pair) % pair).wait_recv()
    whole = parts[0]
    for p in range(1, pair):
        whole = whole + parts[p]
    begin[:, lane_block(group)] = whole
    for q in near_first:
        st_copy(q, group).start()
    for s in range(strips):
        pl.when(strip_direct(s))(b_copy(s).start)
    for g in range(per_row):
        pl.when(c != 2 * g)(a_copy(g).start)
    for g in range(per_row):
        @pl.when(c == 2 * g)
        def _():
            slab[c] = imp_ref[g * LANES : (g + 1) * LANES, :]

    for s in range(strips):
        @pl.when(strip_local(s))
        def _():
            tower[r] = imp_ref[:, lanes_of[s]]

    for i in range(PARTS):
        for slot in range(hops):
            pl.when(relay_used(slot))(functools.partial(pass_on, slot, i))
    for q in range(1, groups):
        st_copy(q, source(q)).wait_recv()

    def orthonormal(block, index):
        def gram_chunk(i, gram):
            at = pl.ds(pl.multiple_of(i * chunk, chunk), chunk)
            h, l = split(block(at))
            res[0, :, at] = h
            res[1, :, at] = l
            both = across(jnp.concatenate([h, l], axis=0), h)
            return gram + (both[:width] + (both[width:] + both[width:].T))

        gram = over(trips, gram_chunk, jnp.zeros((width, width), f32))
        upper, inverse = factor(gram)
        ih, il = split(inverse)
        wide = jnp.concatenate([ih, ih, il], axis=1)

        def solve_chunk(i, carry):
            at = pl.ds(pl.multiple_of(i * chunk, chunk), chunk)
            h = res[0, :, at]
            tall = jnp.concatenate([h, res[1, :, at], h], axis=0)
            h, l = split(jnp.dot(wide, tall, preferred_element_type=f32))
            high[index * width : (index + 1) * width, at] = h
            low[index * width : (index + 1) * width, at] = l
            return carry

        over(trips, solve_chunk, 0)
        return upper

    def first(at):
        return begin[:, at].astype(f32)

    orthonormal(first, 0)

    def a_wait(x):
        pltpu.make_async_remote_copy(
            src_ref=slab.at[x], dst_ref=slab.at[x], send_sem=a_send.at[0], recv_sem=a_recv.at[x],
            device_id=(r, x), device_id_type=MESH,
        ).wait_recv()

    def b_wait(z):
        pltpu.make_async_remote_copy(
            src_ref=tower.at[z], dst_ref=tower.at[z], send_sem=b_send.at[0], recv_sem=b_recv.at[z],
            device_id=(z, c), device_id_type=MESH,
        ).wait_recv()

    for x in range(n_col):
        pl.when(even & (c != x))(functools.partial(a_wait, x))

    @pl.when(even)
    def _():
        for x in range(n_col):
            for i in range(0, cb, LANES):
                spot = x * cb + i
                tower[spot // rows, spot % rows : spot % rows + LANES, :] = slab[x, :, i : i + LANES].T


    def t_wait(z, i):
        where = tower.at[z, part(i)]
        pltpu.make_async_remote_copy(
            src_ref=where, dst_ref=where, send_sem=f_send.at[0, i], recv_sem=f_recv.at[z, i],
            device_id=(z, c), device_id_type=MESH,
        ).wait_recv()

    def t_waits(z):
        for i in range(PARTS):
            t_wait(z, i)

    helper = c - 1 + level % 2
    for z in range(n_row):
        source = mine_at // strips
        far = (z // planes != side) & (source != helper)
        here = (source == c) & (z == r)
        pl.when((k == 1) & far)(functools.partial(t_waits, z))
        pl.when((k == 1) & jnp.logical_not(far) & jnp.logical_not(here))(functools.partial(b_wait, z))
    for q in range(1, pair):
        p_copy(q, member).wait_send()
    for q in range(1, groups):
        st_copy(q, group).wait_send()
    for g in range(per_row):
        pl.when(c != 2 * g)(a_copy(g).wait_send)
    for s in range(strips):
        pl.when(strip_direct(s))(b_copy(s).wait_send)
        pl.when(strip_relayed(s))(functools.partial(sent_strip, s))
    for slot in range(hops):
        pl.when(relay_used(slot))(functools.partial(passed_on, slot))

    offsets = [(dz, dc) for dz in reversed(range(planes)) for dc in reversed(range(n_col)) if dz or dc]
    offsets.sort(key=lambda to: (-to[0] - (to[1] // 2).bit_count(), to[0], -to[1]))

    def i_copy(par, dz, dc, owner):
        where = image.at[par, :, lane_block(owner)]
        index = dz * n_col + dc
        return pltpu.make_async_remote_copy(
            src_ref=where, dst_ref=where,
            send_sem=i_send.at[par, index], recv_sem=i_recv.at[par, index],
            device_id=(side * planes + shift(level, dz, planes), shift(c, dc, n_col)),
            device_id_type=MESH,
        )

    def i_wait(par, dz, dc):
        z = side * planes + shift(level, dz, planes, -1)
        i_copy(par, dz, dc, owned(z, shift(c, dc, n_col, -1))).wait_recv()

    def turn(index):
        at = slice(index * width, (index + 1) * width)
        own = lane_block(group)
        value = high[at, own].astype(f32) + low[at, own].astype(f32)
        out = value[:, :share]
        for i in range(1, pair):
            out = jnp.where(member == i, value[:, i * share : (i + 1) * share], out)
        basis_ref[at, :] = out

    for step in range(STEPS):
        par = step % 2
        seen = (step + 1) * width
        now = slice(step * width, seen)

        mine = jnp.zeros((width, LANES), f32)
        for z in range(n_row):
            mine = mine + jnp.dot(
                high[now, z * rows : (z + 1) * rows], tower[z], preferred_element_type=f32
            )
        image[par, :, lane_block(mine_at)] = mine.astype(image.dtype)
        for dz, dc in offsets:
            i_copy(par, dz, dc, mine_at).start()
        turn(step)
        coeffs = jnp.zeros((width, seen), f32)
        for dz in range(planes):
            for there in [dc for z, dc in reversed(offsets) if z == dz]:
                i_wait(par, dz, there)
            base = shift(level, dz, planes, -1)
            spots = [row_block(side * planes + base)]
            size = share_of * LANES
            for i in range(planes):
                far = ((1 - side) * planes + i) * per_row + base * share_of
                spots.append(pl.ds(pl.multiple_of(far * LANES, size), size))
            for at in spots:
                h = image[par, :, at]
                coeffs = coeffs + across(h, high[:seen, at]) + across(h, low[:seen, at])
        ch, cl = split(coeffs)
        c_both = jnp.concatenate([ch, cl], axis=0)

        def residual(at):
            both = jnp.dot(c_both, high[:seen, at], preferred_element_type=f32)
            fix = jnp.dot(ch, low[:seen, at], preferred_element_type=f32)
            return image[par, :, at].astype(f32) - (both[:width] + both[width:] + fix)

        beta_ref[step] = orthonormal(residual, step + 1)
        alpha_ref[step] = coeffs[:, step * width : seen].T
        for dz, dc in offsets:
            i_copy(par, dz, dc, mine_at).wait_send()

    turn(STEPS)


def local(impedance, start):
    n_row, n_col = lax.axis_size("row"), lax.axis_size("col")
    share, width = start.shape
    pair = LANES // share
    total = share * n_row * n_col
    groups = total // LANES
    blocks = (STEPS + 1) * width
    hops = max(n_row // 4, 1)
    vmem = pl.BlockSpec(memory_space=pltpu.VMEM)
    dma = pltpu.SemaphoreType.DMA
    basis, alphas, betas = pl.pallas_call(
        functools.partial(kernel, n_row, n_col, pair),
        out_shape=(
            jax.ShapeDtypeStruct((blocks, share), f32),
            jax.ShapeDtypeStruct((STEPS, width, width), f32),
            jax.ShapeDtypeStruct((STEPS, width, width), f32),
        ),
        in_specs=[pl.BlockSpec(memory_space=pl.ANY), vmem],
        out_specs=(vmem, vmem, vmem),
        scratch_shapes=[
            pltpu.VMEM(impedance.shape, bf16),
            pltpu.VMEM((width, LANES), bf16),
            pltpu.VMEM((n_col, LANES, impedance.shape[1]), bf16),
            pltpu.VMEM((n_row, impedance.shape[0], LANES), bf16),
            pltpu.VMEM((hops, impedance.shape[0], LANES), bf16),
            pltpu.VMEM((pair, width, LANES), bf16),
            pltpu.VMEM((width, total), bf16),
            pltpu.VMEM((2, width, total), bf16),
            pltpu.VMEM((blocks, total), bf16),
            pltpu.VMEM((blocks, total), bf16),
            pltpu.VMEM((2, width, total), bf16),
            dma((n_col // 2,)), dma((n_col,)),
            dma((impedance.shape[1] // LANES,)), dma((n_row,)),
            dma((impedance.shape[1] // LANES, PARTS)), dma((hops, PARTS)),
            dma((hops, PARTS)), dma((n_row, PARTS)), dma,
            dma((pair,)), dma((pair,)),
            dma((groups,)), dma((groups,)),
            dma((2, groups)), dma((2, groups)),
        ],
        compiler_params=pltpu.CompilerParams(
            collective_id=0, has_side_effects=True, vmem_limit_bytes=60 * 1024 * 1024
        ),
    )(impedance, start.T)
    return basis.T, alphas, betas


def solution(mesh):
    return jax.shard_map(
        local,
        mesh=mesh,
        in_specs=(P("row", "col"), P(("row", "col"), None)),
        out_specs=(P(("row", "col"), None), P(), P()),
        check_vma=False,
    )
```
